32 devices in a mesh: shot: 4 (over y, core), tile: 8 (over z, x).
Axes of the slice: x: 2, y: 2, z: 4, core: 2. Of those that a mesh axis runs over, the one named last changes fastest.
Arguments:
- source: bfloat16 [64, 1, 32, 32, 128], P(('shot', 'tile')), may hold values from -6 to 6
- receiver: bfloat16 [64, 1, 32, 32, 128], P(('shot', 'tile')), may hold values from -6 to 6
- corners: int32 [64, 2], P(('shot', 'tile')), may hold values from 0 to 224, as said below
Outputs:
- filtered: float32 [32, 256, 256], P('tile', 'shot')
The draws below stay inside these ranges and needn't reach their ends.
Inputs may be any that keep to these rules, and one draw needn't show every extreme that they name: corners[s, 0] is at most 224 and corners[s, 1] at most 128, so every box lies inside the image.
All inputs are finite; a program needn't handle non-finite values.
Results may differ from the reference program's by a relative error of at most 0.0003.
Values may be sent and summed in bfloat16 or wider, within the bound.
No kernel may reach another device: no remote copies, remote signals or barrier semaphores. Data moves between devices by JAX's collectives and lax.ppermute only.
A program may use at most 64 MiB of HBM per device.

```python
import jax
import jax.numpy as jnp
from jax import lax

NT = 1
X = 256
Y = 256
BX = 32
BY = 128
SHOTS = 64
Z = 32


def draw_corners(key, part):
    first_key, second_key = jax.random.split(jax.random.fold_in(key, 17))
    row_start = jax.random.randint(first_key, (SHOTS, 1), 0, X - BX + 1)
    col_start = jax.random.randint(second_key, (SHOTS, 1), 0, Y - BY + 1)
    return jnp.concatenate((row_start, col_start), axis=1).astype(jnp.int32)


def level_of(stream_key, dims, cuts, least, largest):
    factor_of = 1.0
    for axis_at, shards_of in cuts:
        steps = jax.random.uniform(jax.random.fold_in(jax.random.fold_in(stream_key, 6), axis_at), (shards_of,), jnp.float32, least / len(cuts), largest / len(cuts))
        factor_of = factor_of * jnp.repeat(jnp.exp(steps), dims[axis_at] // shards_of).reshape((-1,) + (1,) * (len(dims) - 1 - axis_at))
    return factor_of


def bell_draw(key, dims, spread, reach, cuts=(), kind=jnp.bfloat16):
    result = jax.random.normal(key, dims, jnp.float32) * spread
    if len(cuts) > 0:
        result = level_of(key, dims, cuts, -0.22, 0.18) * result
    return jnp.clip(result, min=-reach, max=reach).astype(kind)


def setup_inputs(seed: int = 0) -> dict:
    keys = jax.random.split(jax.random.key(seed), 4)
    return {
        "source": bell_draw(keys[0], (SHOTS, NT, Z, BX, BY), 1.0, 6.0, ((0, 32),)),
        "receiver": bell_draw(keys[1], (SHOTS, NT, Z, BX, BY), 1.0, 6.0, ((0, 32),)),
        "corners": draw_corners(jax.random.fold_in(keys[3], 71), 0),
    }


damping = 1.0


def reference(source, receiver, corners):
    def place(shot, totals):
        image, lights = totals
        wave = lax.dynamic_index_in_dim(source, shot, 0, keepdims=False).astype(jnp.float32)
        back = lax.dynamic_index_in_dim(receiver, shot, 0, keepdims=False).astype(jnp.float32)
        partial_value = jnp.sum(wave * back, axis=0)
        light = jnp.sum(wave * wave, axis=0)
        start = (jnp.int32(0), corners[shot, 0].astype(jnp.int32), corners[shot, 1].astype(jnp.int32))
        image = lax.dynamic_update_slice(image, lax.dynamic_slice(image, start, (Z, BX, BY)) + partial_value, start)
        lights = lax.dynamic_update_slice(lights, lax.dynamic_slice(lights, start, (Z, BX, BY)) + light, start)
        return image, lights

    empty = jnp.zeros((Z, X, Y), jnp.float32)
    image, lights = lax.fori_loop(0, SHOTS, place, (empty, empty))
    normal = image / (damping + lights)
    padded = jnp.pad(normal, 1)
    beside = padded[2:, 1:-1, 1:-1] + padded[:-2, 1:-1, 1:-1]
    beside = beside + padded[1:-1, 2:, 1:-1] + padded[1:-1, :-2, 1:-1]
    beside = beside + padded[1:-1, 1:-1, 2:] + padded[1:-1, 1:-1, :-2]
    return beside - 6.0 * normal
```

```python
import functools

import jax
import jax.numpy as jnp
from jax import lax
from jax.experimental import pallas as pl
from jax.experimental.pallas import tpu as pltpu
from jax.sharding import Mesh, PartitionSpec as P

X = 256
Y = 256
LANES = 128
CORES = 2
EDGE = 8

damping = 1.0


def whole(count):
    return [pl.BlockSpec(memory_space=pltpu.VMEM)] * count


def place_kernel(dims, corner_ref, spot_ref, got_ref, *refs):
    shots, times, planes, rows, sides, half = dims
    outs, total = refs[:-1], refs[-1]
    senders = got_ref.shape[0]
    field = shots * times * planes * rows
    total[...] = jnp.zeros_like(total)
    lane = lax.broadcasted_iota(jnp.int32, (rows, LANES), 1)

    def one_sender(sender, carry):
        for shot in range(shots):
            row = corner_ref[sender, 2 * shot]
            col = corner_ref[sender, 2 * shot + 1]
            turn = lax.rem(col, LANES)
            first = lane >= col
            sums = []
            for plane in range(planes):
                image = light = None
                for time in range(times):
                    at = ((shot * times + time) * planes + plane) * rows
                    wave = got_ref[sender, at:at + rows, :].astype(jnp.float32)
                    back = got_ref[sender, field + at:field + at + rows, :].astype(jnp.float32)
                    image = wave * back if image is None else image + wave * back
                    light = wave * wave if light is None else light + wave * wave
                sums.append((0, plane, pltpu.roll(image, turn, 1)))
                sums.append((1, plane, pltpu.roll(light, turn, 1)))
            span = pl.ds(row, rows)
            fresh = []
            for kind, plane, value in sums:
                low = total[0, kind, plane, span, :]
                high = total[1, kind, plane, span, :]
                fresh.append((kind, plane, low + jnp.where(first, value, 0.0), high + jnp.where(first, 0.0, value)))
            for kind, plane, low, high in fresh:
                total[0, kind, plane, span, :] = low
                total[1, kind, plane, span, :] = high
        return carry

    lax.fori_loop(0, senders, one_sender, 0)
    side = spot_ref[0]
    slot = lax.broadcasted_iota(jnp.int32, (EDGE, LANES), 0)
    for step, out in enumerate(outs):
        target = lax.rem(side + step, sides)
        start = pl.multiple_of(target * half, half)
        before = pl.multiple_of(lax.max(start - EDGE, 0), EDGE)
        after = pl.multiple_of(lax.min(start + half, X - EDGE), EDGE)
        for kind in range(2):
            for plane in range(planes):
                for tile in range(Y // LANES):
                    lanes = slice(tile * LANES, (tile + 1) * LANES)
                    out[kind, plane, :half, lanes] = total[tile, kind, plane, pl.ds(start, half), :]
                    above = total[tile, kind, plane, pl.ds(before, EDGE), :]
                    below = total[tile, kind, plane, pl.ds(after, EDGE), :]
                    above = jnp.where(target > 0, above, 0.0)
                    below = jnp.where(target < sides - 1, below, 0.0)
                    pair = jnp.where(slot == EDGE - 1, above, jnp.where(slot == 0, below, 0.0))
                    out[kind, plane, half:, lanes] = pair


def normal_kernel(dims, spot_ref, *refs):
    planes, half, parts = dims
    ins, (keep, give, straight, across, whole_ref) = refs[:parts], refs[parts:]
    strip = half // CORES
    core = spot_ref[1]
    image = ins[0][0]
    light = ins[0][1]
    for part in ins[1:]:
        image = image + part[0]
        light = light + part[1]
    whole_ref[...] = image / (damping + light)
    slot = lax.broadcasted_iota(jnp.int32, (EDGE, Y), 0)
    edge_plane = core * (planes - 1)
    for out, lone, which in ((keep, straight, core), (give, across, 1 - core)):
        start = pl.multiple_of(which * strip, strip)
        before = pl.multiple_of(lax.max(start - EDGE, 0), EDGE)
        after = pl.multiple_of(lax.min(start + strip, half - EDGE), EDGE)
        for plane in range(planes):
            out[plane, :strip, :] = whole_ref[plane, pl.ds(start, strip), :]
            far = whole_ref[plane, half:, :]
            above = jnp.where(which > 0, whole_ref[plane, pl.ds(before, EDGE), :], far)
            below = jnp.where(which < CORES - 1, whole_ref[plane, pl.ds(after, EDGE), :], far)
            out[plane, strip:, :] = jnp.where(slot == EDGE - 1, above, jnp.where(slot == 0, below, 0.0))
        lone[...] = whole_ref[edge_plane, pl.ds(start, strip), :]


def laplace_kernel(dims, spot_ref, keep, got, straight, across, out):
    planes, strip = dims
    core = spot_ref[1]
    row = lax.broadcasted_iota(jnp.int32, (strip, Y), 0)
    col = lax.broadcasted_iota(jnp.int32, (strip, Y), 1)

    def lateral(cells):
        body = cells[:strip]
        above = jnp.where(row == 0, cells[strip + EDGE - 1:strip + EDGE], pltpu.roll(body, 1, 0))
        below = jnp.where(row == strip - 1, cells[strip:strip + 1], pltpu.roll(body, strip - 1, 0))
        left = jnp.where(col == 0, 0.0, pltpu.roll(body, 1, 1))
        right = jnp.where(col == Y - 1, 0.0, pltpu.roll(body, Y - 1, 1))
        return above + below + left + right - 6.0 * body

    upper_first = core == 0
    lower = jnp.where(upper_first, across[...], straight[...])
    upper = jnp.where(upper_first, straight[...], across[...])
    depth = planes * CORES
    base = core * planes
    other = (1 - core) * planes
    for ref, at in ((keep, base), (got, other)):
        for plane in range(planes):
            out[at + plane] = lateral(ref[plane])
    for ref, far, at in ((keep, got, base), (got, keep, other)):
        lowest = at == 0
        for plane in range(planes):
            if plane == 0:
                down = jnp.where(lowest, lower, far[planes - 1, :strip, :])
            else:
                down = ref[plane - 1, :strip, :]
            if plane == planes - 1:
                up = jnp.where(lowest, far[0, :strip, :], upper)
            else:
                up = ref[plane + 1, :strip, :]
            out[at + plane] = out[at + plane] + (down + up)


def per_device(source, receiver, corners):
    sides = lax.axis_size("side")
    tiles = lax.axis_size("tile")
    spread = tiles * CORES
    shots, times, depth, rows, cols = source.shape
    planes = depth // spread
    half = X // sides
    strip = half // CORES
    side = lax.axis_index("side")
    core = lax.axis_index("core")
    spot = jnp.stack([side, core]).astype(jnp.int32)

    fields = [
        field.reshape(shots, times, spread, planes, rows, cols).transpose(2, 0, 1, 3, 4, 5).reshape(spread, -1, cols)
        for field in (source, receiver)
    ]
    tag = jnp.pad(corners.astype(jnp.bfloat16).reshape(1, -1), ((0, 15), (0, cols - 2 * shots)))
    tag = jnp.broadcast_to(tag[None], (spread, 16, cols))
    packed = jnp.concatenate(fields + [tag], axis=1)
    got = lax.all_to_all(packed, ("tile", "core"), split_axis=0, concat_axis=0, tiled=True)
    corner_all = got[:, -16, : 2 * shots].astype(jnp.int32)

    smem = pl.BlockSpec(memory_space=pltpu.SMEM)
    part_shape = jax.ShapeDtypeStruct((2, planes, half + EDGE, Y), jnp.float32)
    parts = pl.pallas_call(
        functools.partial(place_kernel, (shots, times, planes, rows, sides, half)),
        out_shape=[part_shape] * sides,
        in_specs=[smem, smem] + whole(1),
        out_specs=whole(sides),
        scratch_shapes=[pltpu.VMEM((Y // LANES, 2, planes, X, LANES), jnp.float32)],
    )(corner_all, spot, got)
    parts = [parts[0]] + [
        lax.ppermute(parts[step], "side", [(i, (i + step) % sides) for i in range(sides)])
        for step in range(1, sides)
    ]

    strip_shape = jax.ShapeDtypeStruct((planes, strip + EDGE, Y), jnp.float32)
    plane_shape = jax.ShapeDtypeStruct((strip, Y), jnp.float32)
    keep, give, straight, across = pl.pallas_call(
        functools.partial(normal_kernel, (planes, half, sides)),
        out_shape=[strip_shape, strip_shape, plane_shape, plane_shape],
        in_specs=[smem] + whole(sides),
        out_specs=whole(4),
        scratch_shapes=[pltpu.VMEM((planes, half + EDGE, Y), jnp.float32)],
    )(spot, *parts)
    at = lambda c, t: c * tiles + t
    swap = [(at(c, t), at(1 - c, t)) for c in range(CORES) for t in range(tiles)]
    along = [(at(0, t), at(0, t - 1)) for t in range(1, tiles)]
    along += [(at(1, t), at(1, t + 1)) for t in range(tiles - 1)]
    cross = [(at(0, t), at(1, t - 1)) for t in range(1, tiles)]
    cross += [(at(1, t), at(0, t + 1)) for t in range(tiles - 1)]
    names = ("core", "tile")
    straight = lax.ppermute(straight, names, along)
    across = lax.ppermute(across, names, cross)
    got_strip = lax.ppermute(give, names, swap)
    return pl.pallas_call(
        functools.partial(laplace_kernel, (planes, strip)),
        out_shape=jax.ShapeDtypeStruct((planes * CORES, strip, Y), jnp.float32),
        in_specs=[smem] + whole(4),
        out_specs=pl.BlockSpec(memory_space=pltpu.VMEM),
    )(spot, keep, got_strip, straight, across)


def solution(mesh):
    shot_count, tile_count = mesh.devices.shape
    fine = Mesh(mesh.devices.reshape(shot_count // CORES, CORES, tile_count), ("side", "core", "tile"))
    split = ("side", "core", "tile")
    return jax.shard_map(
        per_device,
        mesh=fine,
        in_specs=(P(split, None, None, None, None), P(split, None, None, None, None), P(split, None)),
        out_specs=P("tile", ("side", "core"), None),
        check_vma=False,
    )
```

```python
import functools

import jax
import jax.numpy as jnp
from jax import lax
from jax.experimental import pallas as pl
from jax.experimental.pallas import tpu as pltpu
from jax.sharding import Mesh, PartitionSpec as P

X = 256
Y = 256
LANES = 128
CORES = 2
EDGE = 8
GRANT = 12 << 20

damping = 1.0


def whole(count):
    return [pl.BlockSpec(memory_space=pltpu.VMEM)] * count


def place_kernel(dims, corner_ref, spot_ref, got_ref, *refs):
    shots, times, planes, rows, sides, half = dims
    outs, total = refs[:-1], refs[-1]
    senders = got_ref.shape[0]
    field = shots * times * planes * rows
    total[...] = jnp.zeros_like(total)
    lane = lax.broadcasted_iota(jnp.int32, (rows, LANES), 1)

    def one_sender(sender, carry):
        for shot in range(shots):
            row = corner_ref[sender, 2 * shot]
            col = corner_ref[sender, 2 * shot + 1]
            turn = lax.rem(col, LANES)
            first = lane >= col
            sums = []
            for plane in range(planes):
                image = light = None
                for time in range(times):
                    at = ((shot * times + time) * planes + plane) * rows
                    wave = got_ref[sender, at:at + rows, :].astype(jnp.float32)
                    back = got_ref[sender, field + at:field + at + rows, :].astype(jnp.float32)
                    image = wave * back if image is None else image + wave * back
                    light = wave * wave if light is None else light + wave * wave
                sums.append((0, plane, pltpu.roll(image, turn, 1)))
                sums.append((1, plane, pltpu.roll(light, turn, 1)))
            span = pl.ds(row, rows)
            fresh = []
            for kind, plane, value in sums:
                low = total[0, kind, plane, span, :]
                high = total[1, kind, plane, span, :]
                fresh.append((kind, plane, low + jnp.where(first, value, 0.0), high + jnp.where(first, 0.0, value)))
            for kind, plane, low, high in fresh:
                total[0, kind, plane, span, :] = low
                total[1, kind, plane, span, :] = high
        return carry

    lax.fori_loop(0, senders, one_sender, 0)
    side = spot_ref[0]
    slot = lax.broadcasted_iota(jnp.int32, (EDGE, LANES), 0)
    for step, out in enumerate(outs):
        target = lax.rem(side + step, sides)
        start = pl.multiple_of(target * half, half)
        before = pl.multiple_of(lax.max(start - EDGE, 0), EDGE)
        after = pl.multiple_of(lax.min(start + half, X - EDGE), EDGE)
        for kind in range(2):
            for plane in range(planes):
                for tile in range(Y // LANES):
                    lanes = slice(tile * LANES, (tile + 1) * LANES)
                    out[kind, plane, :half, lanes] = total[tile, kind, plane, pl.ds(start, half), :]
                    above = total[tile, kind, plane, pl.ds(before, EDGE), :]
                    below = total[tile, kind, plane, pl.ds(after, EDGE), :]
                    above = jnp.where(target > 0, above, 0.0)
                    below = jnp.where(target < sides - 1, below, 0.0)
                    pair = jnp.where(slot == EDGE - 1, above, jnp.where(slot == 0, below, 0.0))
                    out[kind, plane, half:, lanes] = pair


def normal_kernel(dims, spot_ref, *refs):
    planes, half, parts = dims
    ins, (keep, give, straight, across, whole_ref) = refs[:parts], refs[parts:]
    strip = half // CORES
    core = spot_ref[1]
    image = ins[0][0]
    light = ins[0][1]
    for part in ins[1:]:
        image = image + part[0]
        light = light + part[1]
    whole_ref[...] = image / (damping + light)
    slot = lax.broadcasted_iota(jnp.int32, (EDGE, Y), 0)
    edge_plane = core * (planes - 1)
    for out, lone, which in ((keep, straight, core), (give, across, 1 - core)):
        start = pl.multiple_of(which * strip, strip)
        before = pl.multiple_of(lax.max(start - EDGE, 0), EDGE)
        after = pl.multiple_of(lax.min(start + strip, half - EDGE), EDGE)
        for plane in range(planes):
            out[plane, :strip, :] = whole_ref[plane, pl.ds(start, strip), :]
            far = whole_ref[plane, half:, :]
            above = jnp.where(which > 0, whole_ref[plane, pl.ds(before, EDGE), :], far)
            below = jnp.where(which < CORES - 1, whole_ref[plane, pl.ds(after, EDGE), :], far)
            out[plane, strip:, :] = jnp.where(slot == EDGE - 1, above, jnp.where(slot == 0, below, 0.0))
        lone[...] = whole_ref[edge_plane, pl.ds(start, strip), :]


def laplace_kernel(dims, spot_ref, keep, got, straight, across, out):
    planes, strip = dims
    core = spot_ref[1]
    row = lax.broadcasted_iota(jnp.int32, (strip, Y), 0)
    col = lax.broadcasted_iota(jnp.int32, (strip, Y), 1)

    def lateral(cells):
        body = cells[:strip]
        above = jnp.where(row == 0, cells[strip + EDGE - 1:strip + EDGE], pltpu.roll(body, 1, 0))
        below = jnp.where(row == strip - 1, cells[strip:strip + 1], pltpu.roll(body, strip - 1, 0))
        left = jnp.where(col == 0, 0.0, pltpu.roll(body, 1, 1))
        right = jnp.where(col == Y - 1, 0.0, pltpu.roll(body, Y - 1, 1))
        return above + below + left + right - 6.0 * body

    upper_first = core == 0
    lower = jnp.where(upper_first, across[...], straight[...])
    upper = jnp.where(upper_first, straight[...], across[...])
    depth = planes * CORES
    base = core * planes
    other = (1 - core) * planes
    for ref, at in ((keep, base), (got, other)):
        for plane in range(planes):
            out[at + plane] = lateral(ref[plane])
    for ref, far, at in ((keep, got, base), (got, keep, other)):
        lowest = at == 0
        for plane in range(planes):
            if plane == 0:
                down = jnp.where(lowest, lower, far[planes - 1, :strip, :])
            else:
                down = ref[plane - 1, :strip, :]
            if plane == planes - 1:
                up = jnp.where(lowest, far[0, :strip, :], upper)
            else:
                up = ref[plane + 1, :strip, :]
            out[at + plane] = out[at + plane] + (down + up)


def per_device(source, receiver, corners):
    sides = lax.axis_size("side")
    tiles = lax.axis_size("tile")
    spread = tiles * CORES
    shots, times, depth, rows, cols = source.shape
    planes = depth // spread
    half = X // sides
    strip = half // CORES
    side = lax.axis_index("side")
    core = lax.axis_index("core")
    spot = jnp.stack([side, core]).astype(jnp.int32)

    fields = [
        field.reshape(shots, times, spread, planes, rows, cols).transpose(2, 0, 1, 3, 4, 5).reshape(spread, -1, cols)
        for field in (source, receiver)
    ]
    tag = jnp.pad(corners.astype(jnp.bfloat16).reshape(1, -1), ((0, 15), (0, cols - 2 * shots)))
    tag = jnp.broadcast_to(tag[None], (spread, 16, cols))
    packed = jnp.concatenate(fields + [tag], axis=1)
    got = lax.all_to_all(packed, ("tile", "core"), split_axis=0, concat_axis=0, tiled=True)
    corner_all = got[:, -16, : 2 * shots].astype(jnp.int32)

    smem = pl.BlockSpec(memory_space=pltpu.SMEM)
    part_shape = jax.ShapeDtypeStruct((2, planes, half + EDGE, Y), jnp.float32)
    parts = pl.pallas_call(
        functools.partial(place_kernel, (shots, times, planes, rows, sides, half)),
        out_shape=[part_shape] * sides,
        in_specs=[smem, smem] + whole(1),
        out_specs=whole(sides),
        compiler_params=pltpu.CompilerParams(vmem_limit_bytes=GRANT),
        scratch_shapes=[pltpu.VMEM((Y // LANES, 2, planes, X, LANES), jnp.float32)],
    )(corner_all, spot, got)
    parts = [parts[0]] + [
        lax.ppermute(parts[step], "side", [(i, (i + step) % sides) for i in range(sides)])
        for step in range(1, sides)
    ]

    strip_shape = jax.ShapeDtypeStruct((planes, strip + EDGE, Y), jnp.float32)
    plane_shape = jax.ShapeDtypeStruct((strip, Y), jnp.float32)
    keep, give, straight, across = pl.pallas_call(
        functools.partial(normal_kernel, (planes, half, sides)),
        out_shape=[strip_shape, strip_shape, plane_shape, plane_shape],
        in_specs=[smem] + whole(sides),
        out_specs=whole(4),
        compiler_params=pltpu.CompilerParams(vmem_limit_bytes=GRANT),
        scratch_shapes=[pltpu.VMEM((planes, half + EDGE, Y), jnp.float32)],
    )(spot, *parts)
    at = lambda c, t: c * tiles + t
    swap = [(at(c, t), at(1 - c, t)) for c in range(CORES) for t in range(tiles)]
    along = [(at(0, t), at(0, t - 1)) for t in range(1, tiles)]
    along += [(at(1, t), at(1, t + 1)) for t in range(tiles - 1)]
    cross = [(at(0, t), at(1, t - 1)) for t in range(1, tiles)]
    cross += [(at(1, t), at(0, t + 1)) for t in range(tiles - 1)]
    names = ("core", "tile")
    straight = lax.ppermute(straight, names, along)
    across = lax.ppermute(across, names, cross)
    got_strip = lax.ppermute(give, names, swap)
    return pl.pallas_call(
        functools.partial(laplace_kernel, (planes, strip)),
        out_shape=jax.ShapeDtypeStruct((planes * CORES, strip, Y), jnp.float32),
        in_specs=[smem] + whole(4),
        out_specs=pl.BlockSpec(memory_space=pltpu.VMEM),
        compiler_params=pltpu.CompilerParams(vmem_limit_bytes=GRANT),
    )(spot, keep, got_strip, straight, across)


def solution(mesh):
    shot_count, tile_count = mesh.devices.shape
    fine = Mesh(mesh.devices.reshape(shot_count // CORES, CORES, tile_count), ("side", "core", "tile"))
    split = ("side", "core", "tile")
    return jax.shard_map(
        per_device,
        mesh=fine,
        in_specs=(P(split, None, None, None, None), P(split, None, None, None, None), P(split, None)),
        out_specs=P("tile", ("side", "core"), None),
        check_vma=False,
    )
```

```python
import functools

import jax
import jax.numpy as jnp
from jax import lax
from jax.experimental import pallas as pl
from jax.experimental.pallas import tpu as pltpu
from jax.sharding import Mesh, PartitionSpec as P

X = 256
Y = 256
LANES = 128
CORES = 2
EDGE = 8
GRANT = 12 << 20
COVER = 10 ** 7

damping = 1.0


def whole(count):
    return [pl.BlockSpec(memory_space=pltpu.VMEM)] * count


def place_kernel(dims, corner_ref, spot_ref, got_ref, *refs):
    shots, times, planes, rows, sides, half = dims
    outs, total = refs[:-1], refs[-1]
    senders = got_ref.shape[0]
    field = shots * times * planes * rows
    total[...] = jnp.zeros_like(total)
    lane = lax.broadcasted_iota(jnp.int32, (rows, LANES), 1)

    def one_sender(sender, carry):
        for shot in range(shots):
            row = corner_ref[sender, 2 * shot]
            col = corner_ref[sender, 2 * shot + 1]
            turn = lax.rem(col, LANES)
            first = lane >= col
            sums = []
            for plane in range(planes):
                image = light = None
                for time in range(times):
                    at = ((shot * times + time) * planes + plane) * rows
                    wave = got_ref[sender, at:at + rows, :].astype(jnp.float32)
                    back = got_ref[sender, field + at:field + at + rows, :].astype(jnp.float32)
                    image = wave * back if image is None else image + wave * back
                    light = wave * wave if light is None else light + wave * wave
                sums.append((0, plane, pltpu.roll(image, turn, 1)))
                sums.append((1, plane, pltpu.roll(light, turn, 1)))
            span = pl.ds(row, rows)
            fresh = []
            for kind, plane, value in sums:
                low = total[0, kind, plane, span, :]
                high = total[1, kind, plane, span, :]
                fresh.append((kind, plane, low + jnp.where(first, value, 0.0), high + jnp.where(first, 0.0, value)))
            for kind, plane, low, high in fresh:
                total[0, kind, plane, span, :] = low
                total[1, kind, plane, span, :] = high
        return carry

    lax.fori_loop(0, senders, one_sender, 0)
    side = spot_ref[0]
    core = spot_ref[1]
    strip = half // CORES
    slot = lax.broadcasted_iota(jnp.int32, (EDGE, LANES), 0)
    for step, out in enumerate(outs):
        target = lax.rem(side + step // CORES, sides) * CORES + lax.rem(core + step % CORES, CORES)
        start = pl.multiple_of(target * strip, strip)
        before = pl.multiple_of(lax.max(start - EDGE, 0), EDGE)
        after = pl.multiple_of(lax.min(start + strip, X - EDGE), EDGE)
        for kind in range(2):
            for plane in range(planes):
                for tile in range(Y // LANES):
                    lanes = slice(tile * LANES, (tile + 1) * LANES)
                    out[kind, plane, :strip, lanes] = total[tile, kind, plane, pl.ds(start, strip), :]
                    above = total[tile, kind, plane, pl.ds(before, EDGE), :]
                    below = total[tile, kind, plane, pl.ds(after, EDGE), :]
                    above = jnp.where(target > 0, above, 0.0)
                    below = jnp.where(target < sides * CORES - 1, below, 0.0)
                    pair = jnp.where(slot == EDGE - 1, above, jnp.where(slot == 0, below, 0.0))
                    out[kind, plane, strip:, lanes] = pair


def pack_kernel(corner_ref, source, receiver, out, sems):
    shots, times, spread, planes, rows, cols = source.shape
    cell = planes * rows
    copies = []
    for kind, field in enumerate((source, receiver)):
        for shot in range(shots):
            for time in range(times):
                block = (kind * shots + shot) * times + time
                for plane in range(planes):
                    at = block * cell + plane * rows
                    copy = pltpu.make_async_copy(
                        field.at[shot, time, :, plane], out.at[:, at:at + rows, :], sems.at[block * planes + plane]
                    )
                    copy.start()
                    copies.append(copy)
    lane = lax.broadcasted_iota(jnp.int32, (2 * EDGE, cols), 1)
    tag = jnp.zeros((2 * EDGE, cols), jnp.float32)
    for shot in range(shots):
        for which in range(2):
            tag = jnp.where(lane == 2 * shot + which, corner_ref[shot, which].astype(jnp.float32), tag)
    tag = tag.astype(jnp.bfloat16)
    end = 2 * shots * times * cell
    for target in range(spread):
        out[target, end:, :] = tag
    for copy in copies:
        copy.wait()


def normal_kernel(dims, spot_ref, *refs):
    planes, strip, parts = dims
    ins, (cells, low, high) = refs[:parts], refs[parts:]
    core = spot_ref[1]
    for turn in range(CORES):
        base = lax.rem(core + turn, CORES) * planes
        image = ins[turn][0]
        light = ins[turn][1]
        for part in ins[turn + CORES::CORES]:
            image = image + part[0]
            light = light + part[1]
        normal = image / (damping + light)
        for plane in range(planes):
            cells[base + plane] = normal[plane]
    low[...] = cells[0, :strip, :]
    high[...] = cells[planes * CORES - 1, :strip, :]


def lateral_kernel(dims, cells, out):
    depth, strip = dims
    row = lax.broadcasted_iota(jnp.int32, (strip, Y), 0)
    col = lax.broadcasted_iota(jnp.int32, (strip, Y), 1)
    for plane in range(depth):
        body = cells[plane, :strip, :]
        above = jnp.where(row == 0, cells[plane, strip + EDGE - 1:, :], pltpu.roll(body, 1, 0))
        below = jnp.where(row == strip - 1, cells[plane, strip:strip + 1, :], pltpu.roll(body, strip - 1, 0))
        left = jnp.where(col == 0, 0.0, pltpu.roll(body, 1, 1))
        right = jnp.where(col == Y - 1, 0.0, pltpu.roll(body, Y - 1, 1))
        value = above + below + left + right - 6.0 * body
        if plane > 0:
            value = value + cells[plane - 1, :strip, :]
        if plane < depth - 1:
            value = value + cells[plane + 1, :strip, :]
        out[plane] = value


def faces_kernel(inner, under, over, out):
    depth = inner.shape[0]
    for plane in range(depth):
        value = inner[plane]
        if plane == 0:
            value = value + under[...]
        if plane == depth - 1:
            value = value + over[...]
        out[plane] = value


def per_device(source, receiver, corners):
    sides = lax.axis_size("side")
    tiles = lax.axis_size("tile")
    spread = tiles * CORES
    shots, times, depth, rows, cols = source.shape
    planes = depth // spread
    half = X // sides
    strip = half // CORES
    side = lax.axis_index("side")
    core = lax.axis_index("core")
    spot = jnp.stack([side, core]).astype(jnp.int32)
    smem = pl.BlockSpec(memory_space=pltpu.SMEM)
    params = pltpu.CompilerParams(vmem_limit_bytes=GRANT)

    blocks = 2 * shots * times * planes
    raw = [field.reshape(shots, times, spread, planes, rows, cols) for field in (source, receiver)]
    packed = pl.pallas_call(
        pack_kernel,
        out_shape=jax.ShapeDtypeStruct((spread, blocks * rows + 2 * EDGE, cols), jnp.bfloat16),
        in_specs=[smem] + [pl.BlockSpec(memory_space=pltpu.HBM)] * 2,
        out_specs=pl.BlockSpec(memory_space=pltpu.VMEM),
        scratch_shapes=[pltpu.SemaphoreType.DMA((blocks,))],
        compiler_params=params,
    )(corners, *raw)
    got = lax.all_to_all(packed, ("tile", "core"), split_axis=0, concat_axis=0, tiled=True)
    corner_all = got[:, -2 * EDGE, : 2 * shots].astype(jnp.int32)

    group = sides * CORES
    parts = pl.pallas_call(
        functools.partial(place_kernel, (shots, times, planes, rows, sides, half)),
        out_shape=[jax.ShapeDtypeStruct((2, planes, strip + EDGE, Y), jnp.float32)] * group,
        in_specs=[smem, smem] + whole(1),
        out_specs=whole(group),
        compiler_params=params,
        scratch_shapes=[pltpu.VMEM((Y // LANES, 2, planes, X, LANES), jnp.float32)],
    )(corner_all, spot, got)
    moved = [parts[0]]
    for step in range(1, group):
        pairs = [
            (s * CORES + c, (s + step // CORES) % sides * CORES + (c + step) % CORES)
            for s in range(sides)
            for c in range(CORES)
        ]
        moved.append(lax.ppermute(parts[step], ("side", "core"), pairs))

    face = jax.ShapeDtypeStruct((strip, Y), jnp.float32)
    cells, low, high = pl.pallas_call(
        functools.partial(normal_kernel, (planes, strip, group)),
        out_shape=[jax.ShapeDtypeStruct((planes * CORES, strip + EDGE, Y), jnp.float32), face, face],
        in_specs=[smem] + whole(group),
        out_specs=whole(3),
        compiler_params=params,
    )(spot, *moved)
    under = lax.ppermute(high, "tile", [(t, t + 1) for t in range(tiles - 1)])
    over = lax.ppermute(low, "tile", [(t + 1, t) for t in range(tiles - 1)])
    inner_shape = jax.ShapeDtypeStruct((planes * CORES, strip, Y), jnp.float32)
    inner = pl.pallas_call(
        functools.partial(lateral_kernel, (planes * CORES, strip)),
        out_shape=inner_shape,
        in_specs=whole(1),
        out_specs=whole(1)[0],
        compiler_params=params,
        cost_estimate=pl.CostEstimate(flops=COVER, bytes_accessed=1 << 20, transcendentals=0),
    )(cells)
    return pl.pallas_call(
        faces_kernel,
        out_shape=inner_shape,
        in_specs=whole(3),
        out_specs=whole(1)[0],
        compiler_params=params,
    )(inner, under, over)


def solution(mesh):
    shot_count, tile_count = mesh.devices.shape
    fine = Mesh(mesh.devices.reshape(shot_count // CORES, CORES, tile_count), ("side", "core", "tile"))
    split = ("side", "core", "tile")
    return jax.shard_map(
        per_device,
        mesh=fine,
        in_specs=(P(split, None, None, None, None), P(split, None, None, None, None), P(split, None)),
        out_specs=P("tile", ("side", "core"), None),
        check_vma=False,
    )
```

```python
import functools

import jax
import jax.numpy as jnp
from jax import lax
from jax.experimental import pallas as pl
from jax.experimental.pallas import tpu as pltpu
from jax.sharding import Mesh, PartitionSpec as P

X = 256
Y = 256
LANES = 128
CORES = 2
EDGE = 8
GRANT = 12 << 20

damping = 1.0


def whole(count):
    return [pl.BlockSpec(memory_space=pltpu.VMEM)] * count


def place_kernel(dims, corner_ref, spot_ref, got_ref, *refs):
    shots, times, planes, rows, sides, half = dims
    outs, total = refs[:-1], refs[-1]
    outs = list(zip(outs[::2], outs[1::2]))
    senders = got_ref.shape[0]
    field = shots * times * planes * rows
    total[...] = jnp.zeros_like(total)
    lane = lax.broadcasted_iota(jnp.int32, (rows, LANES), 1)

    def one_sender(sender, carry):
        for shot in range(shots):
            row = corner_ref[sender, 2 * shot]
            col = corner_ref[sender, 2 * shot + 1]
            turn = lax.rem(col, LANES)
            first = lane >= col
            sums = []
            for plane in range(planes):
                image = light = None
                for time in range(times):
                    at = ((shot * times + time) * planes + plane) * rows
                    wave = got_ref[sender, at:at + rows, :].astype(jnp.float32)
                    back = got_ref[sender, field + at:field + at + rows, :].astype(jnp.float32)
                    image = wave * back if image is None else image + wave * back
                    light = wave * wave if light is None else light + wave * wave
                sums.append((0, plane, pltpu.roll(image, turn, 1)))
                sums.append((1, plane, pltpu.roll(light, turn, 1)))
            span = pl.ds(row, rows)
            fresh = []
            for kind, plane, value in sums:
                low = total[0, kind, plane, span, :]
                high = total[1, kind, plane, span, :]
                fresh.append((kind, plane, low + jnp.where(first, value, 0.0), high + jnp.where(first, 0.0, value)))
            for kind, plane, low, high in fresh:
                total[0, kind, plane, span, :] = low
                total[1, kind, plane, span, :] = high
        return carry

    lax.fori_loop(0, senders, one_sender, 0)
    side = spot_ref[0]
    core = spot_ref[1]
    strip = half // CORES
    slot = lax.broadcasted_iota(jnp.int32, (EDGE, LANES), 0)
    for step, (outer, inner) in enumerate(outs):
        target = lax.rem(side + step // CORES, sides) * CORES + lax.rem(core + step % CORES, CORES)
        start = pl.multiple_of(target * strip, strip)
        before = pl.multiple_of(lax.max(start - EDGE, 0), EDGE)
        after = pl.multiple_of(lax.min(start + strip, X - EDGE), EDGE)
        moves = [(outer, 0, core * (planes - 1))]
        moves += [(inner, at, at + 1 - core) for at in range(planes - 1)]
        for kind in range(2):
            for out, at, plane in moves:
                for tile in range(Y // LANES):
                    lanes = slice(tile * LANES, (tile + 1) * LANES)
                    out[kind, at, :strip, lanes] = total[tile, kind, plane, pl.ds(start, strip), :]
                    above = total[tile, kind, plane, pl.ds(before, EDGE), :]
                    below = total[tile, kind, plane, pl.ds(after, EDGE), :]
                    above = jnp.where(target > 0, above, 0.0)
                    below = jnp.where(target < sides * CORES - 1, below, 0.0)
                    pair = jnp.where(slot == EDGE - 1, above, jnp.where(slot == 0, below, 0.0))
                    out[kind, at, strip:, lanes] = pair


def pack_kernel(corner_ref, source, receiver, out, sems):
    shots, times, spread, planes, rows, cols = source.shape
    cell = planes * rows
    copies = []
    for kind, field in enumerate((source, receiver)):
        for shot in range(shots):
            for time in range(times):
                block = (kind * shots + shot) * times + time
                for plane in range(planes):
                    at = block * cell + plane * rows
                    copy = pltpu.make_async_copy(
                        field.at[shot, time, :, plane], out.at[:, at:at + rows, :], sems.at[block * planes + plane]
                    )
                    copy.start()
                    copies.append(copy)
    lane = lax.broadcasted_iota(jnp.int32, (2 * EDGE, cols), 1)
    tag = jnp.zeros((2 * EDGE, cols), jnp.float32)
    for shot in range(shots):
        for which in range(2):
            tag = jnp.where(lane == 2 * shot + which, corner_ref[shot, which].astype(jnp.float32), tag)
    tag = tag.astype(jnp.bfloat16)
    end = 2 * shots * times * cell
    for target in range(spread):
        out[target, end:, :] = tag
    for copy in copies:
        copy.wait()


def normal_of(ins, turn):
    image = ins[turn][0]
    light = ins[turn][1]
    for part in ins[turn + CORES::CORES]:
        image = image + part[0]
        light = light + part[1]
    return image / (damping + light)


def outer_kernel(dims, spot_ref, *refs):
    strip, parts = dims
    ins, (ends, low, high) = refs[:parts], refs[parts:]
    core = spot_ref[1]
    for turn in range(CORES):
        ends[lax.rem(core + turn, CORES)] = normal_of(ins, turn)[0]
    low[...] = ends[0, :strip, :]
    high[...] = ends[1, :strip, :]


def laplace_kernel(dims, spot_ref, ends, under, over, *refs):
    planes, strip, parts = dims
    ins, (out, cells) = refs[:parts], refs[parts:]
    depth = planes * CORES
    core = spot_ref[1]
    cells[0] = ends[0]
    cells[depth - 1] = ends[1]
    for turn in range(CORES):
        normal = normal_of(ins, turn)
        base = lax.rem(core + turn, CORES) * (planes - 1) + 1
        for plane in range(planes - 1):
            cells[base + plane] = normal[plane]
    row = lax.broadcasted_iota(jnp.int32, (strip, Y), 0)
    col = lax.broadcasted_iota(jnp.int32, (strip, Y), 1)
    for plane in range(depth):
        body = cells[plane, :strip, :]
        above = jnp.where(row == 0, cells[plane, strip + EDGE - 1:, :], pltpu.roll(body, 1, 0))
        below = jnp.where(row == strip - 1, cells[plane, strip:strip + 1, :], pltpu.roll(body, strip - 1, 0))
        left = jnp.where(col == 0, 0.0, pltpu.roll(body, 1, 1))
        right = jnp.where(col == Y - 1, 0.0, pltpu.roll(body, Y - 1, 1))
        down = under[...] if plane == 0 else cells[plane - 1, :strip, :]
        up = over[...] if plane == depth - 1 else cells[plane + 1, :strip, :]
        out[plane] = above + below + left + right + down + up - 6.0 * body


def per_device(source, receiver, corners):
    sides = lax.axis_size("side")
    tiles = lax.axis_size("tile")
    spread = tiles * CORES
    shots, times, depth, rows, cols = source.shape
    planes = depth // spread
    half = X // sides
    strip = half // CORES
    side = lax.axis_index("side")
    core = lax.axis_index("core")
    spot = jnp.stack([side, core]).astype(jnp.int32)
    smem = pl.BlockSpec(memory_space=pltpu.SMEM)
    params = pltpu.CompilerParams(vmem_limit_bytes=GRANT)

    blocks = 2 * shots * times * planes
    raw = [field.reshape(shots, times, spread, planes, rows, cols) for field in (source, receiver)]
    packed = pl.pallas_call(
        pack_kernel,
        out_shape=jax.ShapeDtypeStruct((spread, blocks * rows + 2 * EDGE, cols), jnp.bfloat16),
        in_specs=[smem] + [pl.BlockSpec(memory_space=pltpu.HBM)] * 2,
        out_specs=pl.BlockSpec(memory_space=pltpu.VMEM),
        scratch_shapes=[pltpu.SemaphoreType.DMA((blocks,))],
    )(corners, *raw)
    got = lax.all_to_all(packed, ("tile", "core"), split_axis=0, concat_axis=0, tiled=True)
    corner_all = got[:, -2 * EDGE, : 2 * shots].astype(jnp.int32)

    group = sides * CORES
    shapes = [
        jax.ShapeDtypeStruct((2, count, strip + EDGE, Y), jnp.float32) for count in (1, planes - 1)
    ]
    parts = pl.pallas_call(
        functools.partial(place_kernel, (shots, times, planes, rows, sides, half)),
        out_shape=shapes * group,
        in_specs=[smem, smem] + whole(1),
        out_specs=whole(2 * group),
        compiler_params=params,
        scratch_shapes=[pltpu.VMEM((Y // LANES, 2, planes, X, LANES), jnp.float32)],
    )(corner_all, spot, got)
    outers, inners = list(parts[::2]), list(parts[1::2])
    for held in (outers, inners):
        for step in range(1, group):
            pairs = [
                (s * CORES + c, (s + step // CORES) % sides * CORES + (c + step) % CORES)
                for s in range(sides)
                for c in range(CORES)
            ]
            held[step] = lax.ppermute(held[step], ("side", "core"), pairs)

    face = jax.ShapeDtypeStruct((strip, Y), jnp.float32)
    ends, low, high = pl.pallas_call(
        functools.partial(outer_kernel, (strip, group)),
        out_shape=[jax.ShapeDtypeStruct((2, strip + EDGE, Y), jnp.float32), face, face],
        in_specs=[smem] + whole(group),
        out_specs=whole(3),
        compiler_params=params,
    )(spot, *outers)
    under = lax.ppermute(high, "tile", [(t, t + 1) for t in range(tiles - 1)])
    over = lax.ppermute(low, "tile", [(t + 1, t) for t in range(tiles - 1)])
    return pl.pallas_call(
        functools.partial(laplace_kernel, (planes, strip, group)),
        out_shape=jax.ShapeDtypeStruct((planes * CORES, strip, Y), jnp.float32),
        in_specs=[smem] + whole(3 + group),
        out_specs=whole(1)[0],
        scratch_shapes=[pltpu.VMEM((planes * CORES, strip + EDGE, Y), jnp.float32)],
        compiler_params=params,
    )(spot, ends, under, over, *inners)


def solution(mesh):
    shot_count, tile_count = mesh.devices.shape
    fine = Mesh(mesh.devices.reshape(shot_count // CORES, CORES, tile_count), ("side", "core", "tile"))
    split = ("side", "core", "tile")
    return jax.shard_map(
        per_device,
        mesh=fine,
        in_specs=(P(split, None, None, None, None), P(split, None, None, None, None), P(split, None)),
        out_specs=P("tile", ("side", "core"), None),
        check_vma=False,
    )
```

```python
import functools

import jax
import jax.numpy as jnp
from jax import lax
from jax.experimental import pallas as pl
from jax.experimental.pallas import tpu as pltpu
from jax.sharding import Mesh, PartitionSpec as P

X = 256
Y = 256
LANES = 128
CORES = 2
EDGE = 8
GRANT = 12 << 20

damping = 1.0


def whole(count):
    return [pl.BlockSpec(memory_space=pltpu.VMEM)] * count


def place_kernel(dims, corner_ref, spot_ref, got_ref, *refs):
    shots, times, planes, rows, sides, half = dims
    outs, total = refs[:-1], refs[-1]
    outs = list(zip(outs[::2], outs[1::2]))
    senders = got_ref.shape[0]
    field = shots * times * planes * rows
    total[...] = jnp.zeros_like(total)
    lane = lax.broadcasted_iota(jnp.int32, (rows, LANES), 1)

    def one_sender(sender, carry):
        for shot in range(shots):
            row = corner_ref[sender, 2 * shot]
            col = corner_ref[sender, 2 * shot + 1]
            turn = lax.rem(col, LANES)
            first = lane >= col
            sums = []
            for plane in range(planes):
                image = light = None
                for time in range(times):
                    at = ((shot * times + time) * planes + plane) * rows
                    wave = got_ref[sender, at:at + rows, :].astype(jnp.float32)
                    back = got_ref[sender, field + at:field + at + rows, :].astype(jnp.float32)
                    image = wave * back if image is None else image + wave * back
                    light = wave * wave if light is None else light + wave * wave
                sums.append((0, plane, pltpu.roll(image, turn, 1)))
                sums.append((1, plane, pltpu.roll(light, turn, 1)))
            span = pl.ds(row, rows)
            fresh = []
            for kind, plane, value in sums:
                low = total[0, kind, plane, span, :]
                high = total[1, kind, plane, span, :]
                fresh.append((kind, plane, low + jnp.where(first, value, 0.0), high + jnp.where(first, 0.0, value)))
            for kind, plane, low, high in fresh:
                total[0, kind, plane, span, :] = low
                total[1, kind, plane, span, :] = high
        return carry

    lax.fori_loop(0, senders, one_sender, 0)
    side = spot_ref[0]
    core = spot_ref[1]
    strip = half // CORES
    slot = lax.broadcasted_iota(jnp.int32, (EDGE, LANES), 0)
    for step, (outer, inner) in enumerate(outs):
        target = lax.rem(side + step // CORES, sides) * CORES + lax.rem(core + step % CORES, CORES)
        start = pl.multiple_of(target * strip, strip)
        before = pl.multiple_of(lax.max(start - EDGE, 0), EDGE)
        after = pl.multiple_of(lax.min(start + strip, X - EDGE), EDGE)
        moves = [(outer, 0, core * (planes - 1))]
        moves += [(inner, at, at + 1 - core) for at in range(planes - 1)]
        for kind in range(2):
            for out, at, plane in moves:
                for tile in range(Y // LANES):
                    lanes = slice(tile * LANES, (tile + 1) * LANES)
                    out[kind, at, :strip, lanes] = total[tile, kind, plane, pl.ds(start, strip), :]
                    above = total[tile, kind, plane, pl.ds(before, EDGE), :]
                    below = total[tile, kind, plane, pl.ds(after, EDGE), :]
                    above = jnp.where(target > 0, above, 0.0)
                    below = jnp.where(target < sides * CORES - 1, below, 0.0)
                    pair = jnp.where(slot == EDGE - 1, above, jnp.where(slot == 0, below, 0.0))
                    out[kind, at, strip:, lanes] = pair


def pack_kernel(corner_ref, source, receiver, out, sems):
    shots, times, spread, cell, cols = source.shape
    copies = []
    for kind, field in enumerate((source, receiver)):
        for shot in range(shots):
            for time in range(times):
                block = (kind * shots + shot) * times + time
                copy = pltpu.make_async_copy(
                    field.at[shot, time], out.at[:, block * cell:(block + 1) * cell, :], sems.at[block]
                )
                copy.start()
                copies.append(copy)
    lane = lax.broadcasted_iota(jnp.int32, (2 * EDGE, cols), 1)
    tag = jnp.zeros((2 * EDGE, cols), jnp.float32)
    for shot in range(shots):
        for which in range(2):
            tag = jnp.where(lane == 2 * shot + which, corner_ref[shot, which].astype(jnp.float32), tag)
    tag = tag.astype(jnp.bfloat16)
    end = 2 * shots * times * cell
    for target in range(spread):
        out[target, end:, :] = tag
    for copy in copies:
        copy.wait()


def normal_of(ins, turn):
    image = ins[turn][0]
    light = ins[turn][1]
    for part in ins[turn + CORES::CORES]:
        image = image + part[0]
        light = light + part[1]
    return image / (damping + light)


def outer_kernel(dims, spot_ref, *refs):
    strip, parts = dims
    ins, (ends, first, second) = refs[:parts], refs[parts:]
    core = spot_ref[1]
    odd = spot_ref[2]
    for turn in range(CORES):
        ends[lax.rem(core + turn, CORES)] = normal_of(ins, turn)[0]
    first[...] = ends[1 - odd, :strip, :]
    second[...] = ends[odd, :strip, :]


def laplace_kernel(dims, spot_ref, ends, first, second, *refs):
    planes, strip, parts = dims
    ins, (out, cells) = refs[:parts], refs[parts:]
    depth = planes * CORES
    core = spot_ref[1]
    even = spot_ref[2] == 0
    under = jnp.where(even, second[...], first[...])
    over = jnp.where(even, first[...], second[...])
    cells[0] = ends[0]
    cells[depth - 1] = ends[1]
    for turn in range(CORES):
        normal = normal_of(ins, turn)
        base = lax.rem(core + turn, CORES) * (planes - 1) + 1
        for plane in range(planes - 1):
            cells[base + plane] = normal[plane]
    row = lax.broadcasted_iota(jnp.int32, (strip, Y), 0)
    col = lax.broadcasted_iota(jnp.int32, (strip, Y), 1)
    for plane in range(depth):
        body = cells[plane, :strip, :]
        above = jnp.where(row == 0, cells[plane, strip + EDGE - 1:, :], pltpu.roll(body, 1, 0))
        below = jnp.where(row == strip - 1, cells[plane, strip:strip + 1, :], pltpu.roll(body, strip - 1, 0))
        left = jnp.where(col == 0, 0.0, pltpu.roll(body, 1, 1))
        right = jnp.where(col == Y - 1, 0.0, pltpu.roll(body, Y - 1, 1))
        down = under if plane == 0 else cells[plane - 1, :strip, :]
        up = over if plane == depth - 1 else cells[plane + 1, :strip, :]
        out[plane] = above + below + left + right + down + up - 6.0 * body


def per_device(source, receiver, corners):
    sides = lax.axis_size("side")
    tiles = lax.axis_size("tile")
    spread = tiles * CORES
    shots, times, depth, rows, cols = source.shape
    planes = depth // spread
    half = X // sides
    strip = half // CORES
    side = lax.axis_index("side")
    core = lax.axis_index("core")
    spot = jnp.stack([side, core, lax.axis_index("tile") % 2]).astype(jnp.int32)
    smem = pl.BlockSpec(memory_space=pltpu.SMEM)
    params = pltpu.CompilerParams(vmem_limit_bytes=GRANT)

    blocks = 2 * shots * times * planes
    raw = [field.reshape(shots, times, spread, planes * rows, cols) for field in (source, receiver)]
    packed = pl.pallas_call(
        pack_kernel,
        out_shape=jax.ShapeDtypeStruct((spread, blocks * rows + 2 * EDGE, cols), jnp.bfloat16),
        in_specs=[smem] + [pl.BlockSpec(memory_space=pltpu.HBM)] * 2,
        out_specs=pl.BlockSpec(memory_space=pltpu.VMEM),
        scratch_shapes=[pltpu.SemaphoreType.DMA((blocks,))],
    )(corners, *raw)
    got = lax.all_to_all(packed, ("tile", "core"), split_axis=0, concat_axis=0, tiled=True)
    corner_all = got[:, -2 * EDGE, : 2 * shots].astype(jnp.int32)

    group = sides * CORES
    shapes = [
        jax.ShapeDtypeStruct((2, count, strip + EDGE, Y), jnp.float32) for count in (1, planes - 1)
    ]
    parts = pl.pallas_call(
        functools.partial(place_kernel, (shots, times, planes, rows, sides, half)),
        out_shape=shapes * group,
        in_specs=[smem, smem] + whole(1),
        out_specs=whole(2 * group),
        compiler_params=params,
        scratch_shapes=[pltpu.VMEM((Y // LANES, 2, planes, X, LANES), jnp.float32)],
    )(corner_all, spot, got)
    outers, inners = list(parts[::2]), list(parts[1::2])
    for held in (outers, inners):
        for step in range(1, group):
            pairs = [
                (s * CORES + c, (s + step // CORES) % sides * CORES + (c + step) % CORES)
                for s in range(sides)
                for c in range(CORES)
            ]
            held[step] = lax.ppermute(held[step], ("side", "core"), pairs)

    face = jax.ShapeDtypeStruct((strip, Y), jnp.float32)
    ends, first, second = pl.pallas_call(
        functools.partial(outer_kernel, (strip, group)),
        out_shape=[jax.ShapeDtypeStruct((2, strip + EDGE, Y), jnp.float32), face, face],
        in_specs=[smem] + whole(group),
        out_specs=whole(3),
        compiler_params=params,
    )(spot, *outers)
    swaps = []
    for begin in range(2):
        meet = [(t, t + 1) for t in range(begin, tiles - 1, 2)]
        swaps.append(meet + [(b, a) for a, b in meet])
    first = lax.ppermute(first, "tile", swaps[0])
    second = lax.ppermute(second, "tile", swaps[1])
    return pl.pallas_call(
        functools.partial(laplace_kernel, (planes, strip, group)),
        out_shape=jax.ShapeDtypeStruct((planes * CORES, strip, Y), jnp.float32),
        in_specs=[smem] + whole(3 + group),
        out_specs=whole(1)[0],
        scratch_shapes=[pltpu.VMEM((planes * CORES, strip + EDGE, Y), jnp.float32)],
        compiler_params=params,
    )(spot, ends, first, second, *inners)


def solution(mesh):
    shot_count, tile_count = mesh.devices.shape
    fine = Mesh(mesh.devices.reshape(shot_count // CORES, CORES, tile_count), ("side", "core", "tile"))
    split = ("side", "core", "tile")
    return jax.shard_map(
        per_device,
        mesh=fine,
        in_specs=(P(split, None, None, None, None), P(split, None, None, None, None), P(split, None)),
        out_specs=P("tile", ("side", "core"), None),
        check_vma=False,
    )
```

```python
import functools

import jax
import jax.numpy as jnp
from jax import lax
from jax.experimental import pallas as pl
from jax.experimental.pallas import tpu as pltpu
from jax.sharding import Mesh, PartitionSpec as P

X = 256
Y = 256
LANES = 128
CORES = 2
EDGE = 8
GRANT = 12 << 20

damping = 1.0


def whole(count):
    return [pl.BlockSpec(memory_space=pltpu.VMEM)] * count


def place_kernel(dims, corner_ref, spot_ref, got_ref, *refs):
    shots, times, planes, rows, sides, half = dims
    outs, total = refs[:-1], refs[-1]
    outs = list(zip(outs[::2], outs[1::2]))
    senders = got_ref.shape[0]
    field = shots * times * planes * rows
    total[...] = jnp.zeros_like(total)
    lane = lax.broadcasted_iota(jnp.int32, (rows, LANES), 1)

    def one_sender(sender, carry):
        for shot in range(shots):
            row = corner_ref[sender, 2 * shot]
            col = corner_ref[sender, 2 * shot + 1]
            turn = lax.rem(col, LANES)
            first = lane >= col
            sums = []
            for plane in range(planes):
                image = light = None
                for time in range(times):
                    at = ((shot * times + time) * planes + plane) * rows
                    wave = got_ref[sender, at:at + rows, :].astype(jnp.float32)
                    back = got_ref[sender, field + at:field + at + rows, :].astype(jnp.float32)
                    image = wave * back if image is None else image + wave * back
                    light = wave * wave if light is None else light + wave * wave
                sums.append((0, plane, pltpu.roll(image, turn, 1)))
                sums.append((1, plane, pltpu.roll(light, turn, 1)))
            span = pl.ds(row, rows)
            fresh = []
            for kind, plane, value in sums:
                low = total[0, kind, plane, span, :]
                high = total[1, kind, plane, span, :]
                fresh.append((kind, plane, low + jnp.where(first, value, 0.0), high + jnp.where(first, 0.0, value)))
            for kind, plane, low, high in fresh:
                total[0, kind, plane, span, :] = low
                total[1, kind, plane, span, :] = high
        return carry

    lax.fori_loop(0, senders, one_sender, 0)
    side = spot_ref[0]
    core = spot_ref[1]
    strip = half // CORES
    slot = lax.broadcasted_iota(jnp.int32, (EDGE, LANES), 0)
    for step, (outer, inner) in enumerate(outs):
        target = lax.rem(side + step // CORES, sides) * CORES + lax.rem(core + step % CORES, CORES)
        start = pl.multiple_of(target * strip, strip)
        before = pl.multiple_of(lax.max(start - EDGE, 0), EDGE)
        after = pl.multiple_of(lax.min(start + strip, X - EDGE), EDGE)
        moves = [(outer, 0, core * (planes - 1))]
        moves += [(inner, at, at + 1 - core) for at in range(planes - 1)]
        for kind in range(2):
            for out, at, plane in moves:
                for tile in range(Y // LANES):
                    lanes = slice(tile * LANES, (tile + 1) * LANES)
                    out[kind, at, :strip, lanes] = total[tile, kind, plane, pl.ds(start, strip), :]
                    above = total[tile, kind, plane, pl.ds(before, EDGE), :]
                    below = total[tile, kind, plane, pl.ds(after, EDGE), :]
                    above = jnp.where(target > 0, above, 0.0)
                    below = jnp.where(target < sides * CORES - 1, below, 0.0)
                    pair = jnp.where(slot == EDGE - 1, above, jnp.where(slot == 0, below, 0.0))
                    out[kind, at, strip:, lanes] = pair


def pack_kernel(corner_ref, source, receiver, out, sems):
    shots, times, spread, cell, cols = source.shape
    copies = []
    for kind, field in enumerate((source, receiver)):
        for shot in range(shots):
            for time in range(times):
                block = (kind * shots + shot) * times + time
                copy = pltpu.make_async_copy(
                    field.at[shot, time], out.at[:, block * cell:(block + 1) * cell, :], sems.at[block]
                )
                copy.start()
                copies.append(copy)
    lane = lax.broadcasted_iota(jnp.int32, (2 * EDGE, cols), 1)
    tag = jnp.zeros((2 * EDGE, cols), jnp.float32)
    for shot in range(shots):
        for which in range(2):
            tag = jnp.where(lane == 2 * shot + which, corner_ref[shot, which].astype(jnp.float32), tag)
    tag = tag.astype(jnp.bfloat16)
    end = 2 * shots * times * cell
    for target in range(spread):
        out[target, end:, :] = tag
    for copy in copies:
        copy.wait()


def normal_of(ins, turn):
    image = ins[turn][0]
    light = ins[turn][1]
    for part in ins[turn + CORES::CORES]:
        image = image + part[0]
        light = light + part[1]
    return image / (damping + light)


def outer_kernel(dims, spot_ref, *refs):
    strip, parts = dims
    ins, (ends, first, second) = refs[:parts], refs[parts:]
    core = spot_ref[1]
    odd = spot_ref[2]
    for turn in range(CORES):
        ends[lax.rem(core + turn, CORES)] = normal_of(ins, turn)[0]
    first[...] = ends[1 - odd, :strip, :]
    second[...] = ends[odd, :strip, :]


def laplace_kernel(dims, spot_ref, ends, first, second, *refs):
    planes, strip, parts = dims
    ins, (out, cells) = refs[:parts], refs[parts:]
    depth = planes * CORES
    core = spot_ref[1]
    even = spot_ref[2] == 0
    under = jnp.where(even, second[...], first[...])
    over = jnp.where(even, first[...], second[...])
    cells[0] = ends[0]
    cells[depth - 1] = ends[1]
    for turn in range(CORES):
        normal = normal_of(ins, turn)
        base = lax.rem(core + turn, CORES) * (planes - 1) + 1
        for plane in range(planes - 1):
            cells[base + plane] = normal[plane]
    row = lax.broadcasted_iota(jnp.int32, (strip, Y), 0)
    col = lax.broadcasted_iota(jnp.int32, (strip, Y), 1)
    for plane in range(depth):
        body = cells[plane, :strip, :]
        above = jnp.where(row == 0, cells[plane, strip + EDGE - 1:, :], pltpu.roll(body, 1, 0))
        below = jnp.where(row == strip - 1, cells[plane, strip:strip + 1, :], pltpu.roll(body, strip - 1, 0))
        left = jnp.where(col == 0, 0.0, pltpu.roll(body, 1, 1))
        right = jnp.where(col == Y - 1, 0.0, pltpu.roll(body, Y - 1, 1))
        down = under if plane == 0 else cells[plane - 1, :strip, :]
        up = over if plane == depth - 1 else cells[plane + 1, :strip, :]
        out[plane] = above + below + left + right + down + up - 6.0 * body


def per_device(source, receiver, corners):
    sides = lax.axis_size("side")
    tiles = lax.axis_size("tile")
    spread = tiles * CORES
    shots, times, depth, rows, cols = source.shape
    planes = depth // spread
    half = X // sides
    strip = half // CORES
    side = lax.axis_index("side")
    core = lax.axis_index("core")
    spot = jnp.stack([side, core, lax.axis_index("tile") % 2]).astype(jnp.int32)
    smem = pl.BlockSpec(memory_space=pltpu.SMEM)
    params = pltpu.CompilerParams(vmem_limit_bytes=GRANT)

    blocks = 2 * shots * times * planes
    raw = [field.reshape(shots, times, spread, planes * rows, cols) for field in (source, receiver)]
    packed = pl.pallas_call(
        pack_kernel,
        out_shape=jax.ShapeDtypeStruct((spread, blocks * rows + 2 * EDGE, cols), jnp.bfloat16),
        in_specs=[smem] + [pl.BlockSpec(memory_space=pltpu.HBM)] * 2,
        out_specs=pl.BlockSpec(memory_space=pltpu.VMEM),
        scratch_shapes=[pltpu.SemaphoreType.DMA((blocks,))],
    )(corners, *raw)
    got = lax.all_to_all(packed, ("tile", "core"), split_axis=0, concat_axis=0, tiled=True)
    corner_all = got[:, -2 * EDGE, : 2 * shots].astype(jnp.int32)

    group = sides * CORES
    shapes = [
        jax.ShapeDtypeStruct((2, count, strip + EDGE, Y), jnp.float32) for count in (1, planes - 1)
    ]
    parts = pl.pallas_call(
        functools.partial(place_kernel, (shots, times, planes, rows, sides, half)),
        out_shape=shapes * group,
        in_specs=[smem, smem] + whole(1),
        out_specs=whole(2 * group),
        compiler_params=params,
        scratch_shapes=[pltpu.VMEM((Y // LANES, 2, planes, X, LANES), jnp.float32)],
    )(corner_all, spot, got)
    outers, inners = list(parts[::2]), list(parts[1::2])
    for held in (outers, inners):
        for step in [*range(CORES, group), *range(1, CORES)]:
            pairs = [
                (s * CORES + c, (s + step // CORES) % sides * CORES + (c + step) % CORES)
                for s in range(sides)
                for c in range(CORES)
            ]
            held[step] = lax.ppermute(held[step], ("side", "core"), pairs)

    face = jax.ShapeDtypeStruct((strip, Y), jnp.float32)
    ends, first, second = pl.pallas_call(
        functools.partial(outer_kernel, (strip, group)),
        out_shape=[jax.ShapeDtypeStruct((2, strip + EDGE, Y), jnp.float32), face, face],
        in_specs=[smem] + whole(group),
        out_specs=whole(3),
        compiler_params=params,
    )(spot, *outers)
    swaps = []
    for begin in range(2):
        meet = [(t, t + 1) for t in range(begin, tiles - 1, 2)]
        swaps.append(meet + [(b, a) for a, b in meet])
    first = lax.ppermute(first, "tile", swaps[0])
    second = lax.ppermute(second, "tile", swaps[1])
    return pl.pallas_call(
        functools.partial(laplace_kernel, (planes, strip, group)),
        out_shape=jax.ShapeDtypeStruct((planes * CORES, strip, Y), jnp.float32),
        in_specs=[smem] + whole(3 + group),
        out_specs=whole(1)[0],
        scratch_shapes=[pltpu.VMEM((planes * CORES, strip + EDGE, Y), jnp.float32)],
        compiler_params=params,
    )(spot, ends, first, second, *inners)


def solution(mesh):
    shot_count, tile_count = mesh.devices.shape
    fine = Mesh(mesh.devices.reshape(shot_count // CORES, CORES, tile_count), ("side", "core", "tile"))
    split = ("side", "core", "tile")
    return jax.shard_map(
        per_device,
        mesh=fine,
        in_specs=(P(split, None, None, None, None), P(split, None, None, None, None), P(split, None)),
        out_specs=P("tile", ("side", "core"), None),
        check_vma=False,
    )
```
